32 devices in a mesh: dp: 8 (over y, x, core), mp: 4 (over z).
Axes of the slice: x: 2, y: 2, z: 4, core: 2. Of those that a mesh axis runs over, the one named last changes fastest.
Arguments:
- train_acts: bfloat16 [4096, 2560], P('dp'), may hold values from -6 to 6
- train_grads: bfloat16 [4096, 2560], P('dp'), may hold values from -6 to 6
- lengths: int32 [32], P('dp'), may hold values from 1 to 256, as said below
- query_acts: bfloat16 [128, 2560], replicated, may hold values from -6 to 6
- query_grads: bfloat16 [128, 2560], replicated, may hold values from -0.0059814453 to 0.0059814453
- basis_in: bfloat16 [2560, 2560], P(None, 'mp'), may hold values from -0.125 to 0.125
- basis_out: bfloat16 [2560, 2560], P(None, 'mp'), may hold values from -0.125 to 0.125
Outputs:
- scores: float32 [1, 32], P(None, 'dp')
The draws below stay inside these ranges and needn't reach their ends.
Inputs may be any that keep to these rules, and one draw needn't show every extreme that they name: The 4 lengths of one index of dp sum to at most 512; in every draw some index's sequences fill all 512 rows and one of them has exactly 256 tokens.
All inputs are finite; a program needn't handle non-finite values.
Results may differ from the reference program's by a relative error of at most 0.0045.
Values may be sent and summed in bfloat16 or wider, within the bound.
A program may use at most 128 MiB of HBM per device.

```python
import jax
import jax.numpy as jnp
from jax import lax

D_IN = 2560
D_OUT = 2560
TOK_CAP = 512
SEQ_DEV = 4
QUERIES = 1
QLEN = 128
SEQ_MAX = 256
TOKENS = 4096
SEQUENCES = 32


def draw_lengths(key, part):
    groups = SEQUENCES // SEQ_DEV
    key_total = jax.random.fold_in(key, 11)
    key_weight = jax.random.fold_in(key, 12)
    key_device = jax.random.fold_in(key, 13)
    key_slot = jax.random.fold_in(key, 14)
    totals = jax.random.randint(key_total, (groups,), TOK_CAP // 4, TOK_CAP - TOK_CAP // 8 + 1)
    weights = jax.random.randint(key_weight, (groups, SEQ_DEV), 1, 3)
    cumulative = jnp.cumsum(weights, axis=1)
    whole = cumulative[:, -1:]
    bounds = totals[:, None] * cumulative // whole
    previous = jnp.concatenate([jnp.zeros((groups, 1), jnp.int32), bounds[:, :-1]], axis=1)
    general = bounds - previous
    full_device = jax.random.randint(key_device, (), 0, groups)
    full_slot = jax.random.randint(key_slot, (), 0, SEQ_DEV)
    slots = jnp.arange(SEQ_DEV, dtype=jnp.int32)
    full_weights = jnp.where(slots == full_slot, 0, weights[full_device])
    full_cumulative = jnp.cumsum(full_weights)
    remainder = TOK_CAP - SEQ_MAX
    full_bounds = remainder * full_cumulative // full_cumulative[-1]
    full_previous = jnp.concatenate([jnp.zeros((1,), jnp.int32), full_bounds[:-1]])
    full_lengths = jnp.where(slots == full_slot, SEQ_MAX, full_bounds - full_previous)
    rows = jnp.arange(groups, dtype=jnp.int32)
    result = jnp.where((rows == full_device)[:, None], full_lengths[None, :], general)
    return result.reshape(SEQUENCES).astype(jnp.int32)


def level_of(stream_key, dims, split, low, top_value):
    loudness = 1.0
    for axis_at, shards_of in split:
        steps = jax.random.uniform(jax.random.fold_in(jax.random.fold_in(stream_key, 6), axis_at), (shards_of,), jnp.float32, low / len(split), top_value / len(split))
        loudness = loudness * jnp.repeat(jnp.exp(steps), dims[axis_at] // shards_of).reshape((-1,) + (1,) * (len(dims) - 1 - axis_at))
    return loudness


def scatter_about(key, shape, deviation, most, split=(), kind=jnp.bfloat16):
    drawn = deviation * jax.random.normal(key, shape, jnp.float32)
    if split:
        drawn = drawn * level_of(key, shape, split, -0.22, 0.18)
    return jnp.clip(drawn, -most, most).astype(kind)


def setup_inputs(seed: int = 0) -> dict:
    streams_of = jax.random.split(jax.random.key(seed), 8)
    return {
        "train_acts": scatter_about(streams_of[0], (TOKENS, D_IN), 1.0, 6.0, ((0, 8),)),
        "train_grads": scatter_about(streams_of[1], (TOKENS, D_OUT), 1.0, 6.0, ((0, 8),)),
        "lengths": draw_lengths(jax.random.fold_in(streams_of[7], 71), 0),
        "query_acts": scatter_about(streams_of[3], (QUERIES * QLEN, D_IN), 1.0, 6.0),
        "query_grads": scatter_about(streams_of[4], (QUERIES * QLEN, D_OUT), 0.001, 0.0059814453),
        "basis_in": scatter_about(streams_of[5], (D_IN, D_IN), D_IN ** -0.5, 0.125, ((1, 4),)),
        "basis_out": scatter_about(streams_of[6], (D_OUT, D_OUT), D_OUT ** -0.5, 0.125, ((1, 4),)),
    }


damping_ratio = 0.1

def rotate(values, basis):
    return jnp.dot(values, basis, preferred_element_type=jnp.float32).astype(jnp.bfloat16)

def reference(train_acts, train_grads, lengths, query_acts, query_grads, basis_in, basis_out):
    groups = SEQUENCES // SEQ_DEV
    acts_rot = rotate(train_acts, basis_in).reshape(groups, TOK_CAP, D_IN)
    grads_rot = rotate(train_grads, basis_out).reshape(groups, TOK_CAP, D_OUT)
    seq_lengths = lengths.reshape(groups, SEQ_DEV).astype(jnp.int32)
    finish = jnp.cumsum(seq_lengths, axis=1).astype(jnp.int32)
    starts = (finish - seq_lengths).astype(jnp.int32)
    position = jnp.arange(SEQ_MAX, dtype=jnp.int32)

    def sequence_grad(index):
        device = (index // SEQ_DEV).astype(jnp.int32)
        slot = (index % SEQ_DEV).astype(jnp.int32)
        first = starts[device, slot]
        last = finish[device, slot]
        begin = jnp.minimum(first, TOK_CAP - SEQ_MAX).astype(jnp.int32)
        grads_win = lax.dynamic_slice_in_dim(grads_rot[device], begin, SEQ_MAX, 0)
        acts_win = lax.dynamic_slice_in_dim(acts_rot[device], begin, SEQ_MAX, 0)
        inside = (position + begin >= first) & (position + begin < last)
        grads_win = jnp.where(inside[:, None], grads_win, jnp.zeros_like(grads_win))
        return jnp.dot(grads_win.T.astype(jnp.float32), acts_win.astype(jnp.float32), preferred_element_type=jnp.float32)

    def add_square(index, running):
        product = sequence_grad(index)
        return running + product * product
    curvature = lax.fori_loop(0, SEQUENCES, add_square, jnp.zeros((D_OUT, D_IN), jnp.float32)) / SEQUENCES
    damping = damping_ratio * jnp.mean(curvature)
    query_g = rotate(query_grads, basis_out).astype(jnp.float32).reshape(QUERIES, QLEN, D_OUT)
    query_a = rotate(query_acts, basis_in).astype(jnp.float32).reshape(QUERIES, QLEN, D_IN)
    query_grad = jnp.einsum('qti,qtj->qij', query_g, query_a)
    precond = (query_grad / (curvature + damping)).astype(jnp.bfloat16)
    precond = lax.optimization_barrier(precond).astype(jnp.float32)

    def score_column(index):
        stored = sequence_grad(index).astype(jnp.bfloat16)
        stored = lax.optimization_barrier(stored).astype(jnp.float32)
        return jnp.einsum('qij,ij->q', precond, stored)
    columns = lax.map(score_column, jnp.arange(SEQUENCES, dtype=jnp.int32))
    return columns.T
```

```python
import functools

import jax
import jax.numpy as jnp
from jax import lax
from jax.experimental import pallas as pl
from jax.experimental.pallas import tpu as pltpu
from jax.sharding import PartitionSpec as P

damping_ratio = 0.1
MESH = pl.DeviceIdType.MESH
VMEM = pl.BlockSpec(memory_space=pltpu.VMEM)
GRANT = 56 * 1024 * 1024


def rotate(values, basis):
    return jnp.dot(values, basis, preferred_element_type=jnp.float32).astype(jnp.bfloat16)


def remote(src, dst, send, recv, d, m):
    return pltpu.make_async_remote_copy(
        src_ref=src, dst_ref=dst, send_sem=send, recv_sem=recv, device_id=(d, m), device_id_type=MESH
    )


def spread_kernel(mp, a, g, q, s, a2, gs, q2, ss, a_send, a_recv, q_send, q_recv, o_send, o_recv):
    d, m = lax.axis_index("dp"), lax.axis_index("mp")
    rows, cols = a.shape
    half = mp // 2
    core = lax.rem(d, 2)
    base = d - core
    sibling = base + 1 - core
    owner = m // half
    place = lax.rem(m, half)

    def a_slot(c, j):
        return a2.at[pl.ds(pl.multiple_of(c * rows, rows), rows), pl.ds(pl.multiple_of(j * cols, cols), cols)]

    def q_slot(j):
        return q2.at[:, pl.ds(pl.multiple_of(j * cols, cols), cols)]

    def a_copy(k):
        return remote(a, a_slot(core, place), a_send.at[k], a_recv.at[core, place], base + owner, lax.rem(m + k, mp))

    def q_copy(k):
        return remote(q, q_slot(place), q_send.at[k], q_recv.at[place], d, lax.rem(m + k, mp))

    g_copy = remote(g, gs, o_send.at[0], o_recv.at[0], sibling, m)
    s_copy = remote(s, ss, o_send.at[1], o_recv.at[1], sibling, m)
    order = [mp // 2] + [k for k in range(1, mp) if k != mp // 2]
    for k in order:
        a_copy(k).start()
    g_copy.start()
    s_copy.start()

    @pl.when(owner == core)
    def _():
        pltpu.make_async_copy(a, a_slot(core, place), a_recv.at[core, place]).start()
        pltpu.make_async_copy(q, q_slot(place), q_recv.at[place]).start()
        for k in order:
            q_copy(k).start()

    @pl.when(owner != core)
    def _():
        a_copy(0).start()

    for c in range(2):
        for j in range(half):
            pltpu.make_async_copy(a, a_slot(c, j), a_recv.at[c, j]).wait()
    for j in range(half):
        pltpu.make_async_copy(q, q_slot(j), q_recv.at[j]).wait()
    for k in range(1, mp):
        a_copy(k).wait_send()

    @pl.when(owner == core)
    def _():
        for k in range(1, mp):
            q_copy(k).wait_send()

    @pl.when(owner != core)
    def _():
        a_copy(0).wait_send()

    g_copy.wait()
    s_copy.wait()


def spread(mp, a, g, q, s):
    rows, cols = a.shape
    half = mp // 2
    dma = pltpu.SemaphoreType.DMA
    return pl.pallas_call(
        functools.partial(spread_kernel, mp),
        out_shape=[
            jax.ShapeDtypeStruct((2 * rows, half * cols), a.dtype),
            jax.ShapeDtypeStruct(g.shape, g.dtype),
            jax.ShapeDtypeStruct((q.shape[0], half * cols), q.dtype),
            jax.ShapeDtypeStruct(s.shape, s.dtype),
        ],
        in_specs=[VMEM] * 4,
        out_specs=[VMEM] * 4,
        scratch_shapes=[dma((mp,)), dma((2, half)), dma((mp,)), dma((half,)), dma((2,)), dma((2,))],
        compiler_params=pltpu.CompilerParams(has_side_effects=True, vmem_limit_bytes=GRANT),
        name="spread",
    )(a, g, q, s)


def square_kernel(slots, g0, g1, a2, c, sums):
    rows = a2.shape[0] // 2
    width = c.shape[0]
    total = None
    for g, at in ((g0, 0), (g1, rows)):
        for slot in range(slots):
            p = jnp.dot(
                g[slot * width:(slot + 1) * width, :], a2[at:at + rows, :], preferred_element_type=jnp.float32
            )
            total = p * p if total is None else total + p * p
    c[...] = total.astype(c.dtype)
    sums[...] = jnp.sum(total, axis=0, keepdims=True)


def squares(slots, g0, g1, a2, tile):
    rows2, cols = a2.shape
    width = g0.shape[0] // slots
    whole = lambda j: (0, 0)
    part = lambda j: (0, j)
    return pl.pallas_call(
        functools.partial(square_kernel, slots),
        grid=(cols // tile,),
        out_shape=[
            jax.ShapeDtypeStruct((width, cols), jnp.bfloat16),
            jax.ShapeDtypeStruct((1, cols), jnp.float32),
        ],
        in_specs=[
            pl.BlockSpec(g0.shape, whole),
            pl.BlockSpec(g1.shape, whole),
            pl.BlockSpec((rows2, tile), part),
        ],
        out_specs=[pl.BlockSpec((width, tile), part), pl.BlockSpec((1, tile), part)],
        compiler_params=pltpu.CompilerParams(vmem_limit_bytes=GRANT),
        name="squares",
    )(g0, g1, a2)


def piece(ref, across, shape, p):
    high, wide = shape
    return ref.at[
        pl.ds(pl.multiple_of((p // across) * high, high), high),
        pl.ds(pl.multiple_of(lax.rem(p, across) * wide, wide), wide),
    ]


def scatter_kernel(n, mp, across, shape, c, t, r, tt, c_send, c_recv, t_send, t_recv, u_send, u_recv):
    d, m = lax.axis_index("dp"), lax.axis_index("mp")
    core = lax.rem(d, 2)
    chip = d // 2
    base = d - core
    near = 2 * mp
    me = core * mp + m

    def c_copy(k):
        p = lax.rem(chip + k, n)
        return remote(piece(c, across, shape, p), r.at[chip], c_send.at[k], c_recv.at[chip], 2 * p + core, m)

    def t_copy(k):
        o = lax.rem(me + k, near)
        return remote(t, tt.at[chip, me], t_send.at[k], t_recv.at[me], base + o // mp, lax.rem(o, mp))

    def u_copy(k):
        p = lax.rem(chip + k, n)
        return remote(tt.at[chip], tt.at[chip], u_send.at[k], u_recv.at[chip], 2 * p + core, m)

    for k in range(1, near):
        t_copy(k).start()
    pltpu.make_async_copy(t, tt.at[chip, me], t_recv.at[me]).start()
    for k in range(1, n):
        c_copy(k).start()
    pltpu.make_async_copy(piece(c, across, shape, chip), r.at[chip], c_recv.at[chip]).start()
    for o in range(near):
        pltpu.make_async_copy(t, tt.at[chip, o], t_recv.at[o]).wait()
    for k in range(1, n):
        u_copy(k).start()
    for k in range(1, near):
        t_copy(k).wait_send()
    for k in range(1, n):
        p = lax.rem(chip + k, n)
        pltpu.make_async_copy(tt.at[chip], tt.at[p], u_recv.at[p]).wait()
        u_copy(k).wait_send()
        c_copy(k).wait_send()
    for p in range(n):
        pltpu.make_async_copy(piece(c, across, shape, chip), r.at[p], c_recv.at[p]).wait()


def scatter(n, mp, across, shape, c, t):
    dma = pltpu.SemaphoreType.DMA
    return pl.pallas_call(
        functools.partial(scatter_kernel, n, mp, across, shape),
        out_shape=[
            jax.ShapeDtypeStruct((n,) + shape, c.dtype),
            jax.ShapeDtypeStruct((n, 2 * mp) + t.shape, t.dtype),
        ],
        in_specs=[VMEM] * 2,
        out_specs=[VMEM] * 2,
        scratch_shapes=[dma((n,)), dma((n,)), dma((2 * mp,)), dma((2 * mp,)), dma((n,)), dma((n,))],
        compiler_params=pltpu.CompilerParams(has_side_effects=True, vmem_limit_bytes=GRANT),
        name="scatter",
    )(c, t)


def collect_kernel(n, across, shape, x, out, send, recv):
    d, m = lax.axis_index("dp"), lax.axis_index("mp")
    core = lax.rem(d, 2)
    chip = d // 2
    here = piece(out, across, shape, chip)

    def copy(k):
        return remote(x, here, send.at[k], recv.at[chip], 2 * lax.rem(chip + k, n) + core, m)

    for k in range(1, n):
        copy(k).start()
    pltpu.make_async_copy(x, here, recv.at[chip]).start()
    for p in range(n):
        pltpu.make_async_copy(x, piece(out, across, shape, p), recv.at[p]).wait()
    for k in range(1, n):
        copy(k).wait_send()


def collect(n, across, shape, full, x):
    dma = pltpu.SemaphoreType.DMA
    return pl.pallas_call(
        functools.partial(collect_kernel, n, across, shape),
        out_shape=jax.ShapeDtypeStruct(full, x.dtype),
        in_specs=[VMEM],
        out_specs=VMEM,
        scratch_shapes=[dma((n,)), dma((n,))],
        compiler_params=pltpu.CompilerParams(has_side_effects=True, vmem_limit_bytes=GRANT),
        name="collect",
    )(x)


def score_kernel(g0, g1, a2, p, out):
    rows = g0.shape[0]

    @pl.when(pl.program_id(0) == 0)
    def _():
        out[...] = jnp.zeros_like(out)

    for g, at in ((g0, 0), (g1, rows)):
        y = jnp.dot(g[...], p[...], preferred_element_type=jnp.float32)
        z = y * a2[at:at + rows, :].astype(jnp.float32)
        total = z[:, :128]
        for lane in range(128, z.shape[1], 128):
            total = total + z[:, lane:lane + 128]
        out[at:at + rows, :] += total


def token_scores(g0, g1, a2, p, tile):
    rows2, cols = a2.shape
    whole = lambda j: (0, 0)
    part = lambda j: (0, j)
    return pl.pallas_call(
        score_kernel,
        grid=(cols // tile,),
        out_shape=jax.ShapeDtypeStruct((rows2, 128), jnp.float32),
        in_specs=[
            pl.BlockSpec(g0.shape, whole),
            pl.BlockSpec(g1.shape, whole),
            pl.BlockSpec((rows2, tile), part),
            pl.BlockSpec((p.shape[0], tile), part),
        ],
        out_specs=pl.BlockSpec((rows2, 128), whole),
        compiler_params=pltpu.CompilerParams(vmem_limit_bytes=GRANT),
        name="token_scores",
    )(g0, g1, a2, p)


def finish_kernel(mp, t, out, send, recv):
    d, m = lax.axis_index("dp"), lax.axis_index("mp")
    core = lax.rem(d, 2)
    base = d - core
    near = 2 * mp
    me = core * mp + m

    def copy(k):
        o = lax.rem(me + k, near)
        return remote(t, out.at[me], send.at[k], recv.at[me], base + o // mp, lax.rem(o, mp))

    for k in range(1, near):
        copy(k).start()
    pltpu.make_async_copy(t, out.at[me], recv.at[me]).start()
    for o in range(near):
        pltpu.make_async_copy(t, out.at[o], recv.at[o]).wait()
    for k in range(1, near):
        copy(k).wait_send()


def share(mp, t):
    dma = pltpu.SemaphoreType.DMA
    return pl.pallas_call(
        functools.partial(finish_kernel, mp),
        out_shape=jax.ShapeDtypeStruct((2 * mp,) + t.shape, t.dtype),
        in_specs=[VMEM],
        out_specs=VMEM,
        scratch_shapes=[dma((2 * mp,)), dma((2 * mp,))],
        compiler_params=pltpu.CompilerParams(has_side_effects=True),
        name="share",
    )(t)


def shards(dp, mp, train_acts, train_grads, lengths, query_acts, query_grads, basis_in, basis_out):
    rows = train_acts.shape[0]
    width = basis_in.shape[1]
    slots = lengths.shape[0]
    n = dp // 2
    cols = (mp // 2) * basis_in.shape[1]
    down = max(
        k for k in range(1, n + 1) if n % k == 0 and width % (8 * k) == 0 and cols % (128 * (n // k)) == 0
    )
    across = n // down
    shape = (width // down, cols // across)
    tile = 256
    core = lax.axis_index("dp") % 2
    chip = lax.axis_index("dp") // 2

    finish = jnp.cumsum(lengths)
    slot_of = jnp.sum(jnp.arange(rows, dtype=jnp.int32)[None, :] >= finish[:, None], axis=0)
    slot_rows = jnp.broadcast_to(slot_of.astype(jnp.float32)[None, :], (8, rows))
    acts_block = rotate(train_acts, basis_in)
    grads_own = rotate(train_grads, basis_out)
    query_block = rotate(query_acts, basis_in)
    query_grot = rotate(query_grads, basis_out)
    acts2, grads_sib, query2, slot_sib = spread(mp, acts_block, grads_own, query_block, slot_rows)

    own_first = core == 0
    grads0 = jnp.where(own_first, grads_own, grads_sib)
    grads1 = jnp.where(own_first, grads_sib, grads_own)
    slot0 = jnp.where(own_first, slot_rows[0], slot_sib[0])
    slot1 = jnp.where(own_first, slot_sib[0], slot_rows[0])
    names = jnp.arange(slots, dtype=jnp.float32)
    mask0 = names[:, None] == slot0[None, :]
    mask1 = names[:, None] == slot1[None, :]

    def masked(grads, mask):
        turned = grads.T
        return jnp.where(mask[:, None, :], turned[None], jnp.zeros_like(turned)[None]).reshape(slots * width, rows)

    squared, sums = squares(slots, masked(grads0, mask0), masked(grads1, mask1), acts2, tile)
    total = jnp.broadcast_to(jnp.sum(sums), (8, 128))
    pieces, totals = scatter(n, mp, across, shape, squared, total)

    sequences = slots * dp
    curvature = jnp.sum(pieces.astype(jnp.float32), axis=0) / sequences
    entries = width * mp * width * mp
    damping = damping_ratio * (jnp.sum(totals[:, :, 0, 0]) / sequences / entries)
    row_at = (chip // across) * shape[0]
    col_at = (chip % across) * shape[1]
    left = lax.dynamic_slice_in_dim(query_grot, row_at, shape[0], 1)
    right = lax.dynamic_slice_in_dim(query2, col_at, shape[1], 1)
    local_grad = lax.dot_general(left, right, (((0,), (0,)), ((), ())), preferred_element_type=jnp.float32)
    precond = (local_grad / (curvature + damping)).astype(jnp.bfloat16)
    precond_full = collect(n, across, shape, (width, cols), precond)

    by_token = jnp.sum(token_scores(grads0, grads1, acts2, precond_full, tile), axis=1)
    partial0 = jnp.sum(jnp.where(mask0, by_token[None, :rows], 0.0), axis=1)
    partial1 = jnp.sum(jnp.where(mask1, by_token[None, rows:], 0.0), axis=1)
    packed = jnp.zeros((8, 128), jnp.float32).at[0, :slots].set(partial0).at[1, :slots].set(partial1)
    summed = jnp.sum(share(mp, packed), axis=0)
    return jnp.where(own_first, summed[0:1, :slots], summed[1:2, :slots])


def solution(mesh):
    return jax.shard_map(
        functools.partial(shards, mesh.shape["dp"], mesh.shape["mp"]),
        mesh=mesh,
        in_specs=(P("dp", None), P("dp", None), P("dp"), P(), P(), P(None, "mp"), P(None, "mp")),
        out_specs=P(None, "dp"),
        check_vma=False,
    )
```

```python
import functools

import jax
import jax.numpy as jnp
from jax import lax
from jax.experimental import pallas as pl
from jax.experimental.pallas import tpu as pltpu
from jax.sharding import PartitionSpec as P

damping_ratio = 0.1
MESH = pl.DeviceIdType.MESH
VMEM = pl.BlockSpec(memory_space=pltpu.VMEM)
GRANT = 56 * 1024 * 1024


def rotate(values, basis):
    return jnp.dot(values, basis, preferred_element_type=jnp.float32).astype(jnp.bfloat16)


def remote(src, dst, send, recv, d, m):
    return pltpu.make_async_remote_copy(
        src_ref=src, dst_ref=dst, send_sem=send, recv_sem=recv, device_id=(d, m), device_id_type=MESH
    )


def spread_kernel(mp, slots, a, g, gt, q, s, a2, g2, q2, s2, sq, sums, gt2, acc, a_send, a_recv, q_send, q_recv, o_send, o_recv):
    d, m = lax.axis_index("dp"), lax.axis_index("mp")
    rows, cols = a.shape
    half = mp // 2
    core = lax.rem(d, 2)
    base = d - core
    sibling = base + 1 - core
    owner = m // half
    place = lax.rem(m, half)

    def a_slot(c, j):
        return a2.at[pl.ds(pl.multiple_of(c * rows, rows), rows), pl.ds(pl.multiple_of(j * cols, cols), cols)]

    def q_slot(j):
        return q2.at[:, pl.ds(pl.multiple_of(j * cols, cols), cols)]

    def a_copy(k):
        return remote(a, a_slot(core, place), a_send.at[k], a_recv.at[core, place], base + owner, lax.rem(m + k, mp))

    def q_copy(k):
        return remote(q, q_slot(place), q_send.at[k], q_recv.at[place], d, lax.rem(m + k, mp))

    pairs = ((gt, gt2), (s, s2), (g, g2))
    order = [mp // 2] + [k for k in range(1, mp) if k != mp // 2]
    for k in order:
        a_copy(k).start()
    for i, (src, dst) in enumerate(pairs):
        remote(src, dst.at[core], o_send.at[i], o_recv.at[i, core], sibling, m).start()
        pltpu.make_async_copy(src, dst.at[core], o_recv.at[i, core]).start()

    @pl.when(owner == core)
    def _():
        pltpu.make_async_copy(a, a_slot(core, place), a_recv.at[core, place]).start()
        pltpu.make_async_copy(q, q_slot(place), q_recv.at[place]).start()
        for k in order:
            q_copy(k).start()

    @pl.when(owner != core)
    def _():
        a_copy(0).start()

    for i, (src, dst) in enumerate(pairs):
        for c in range(2):
            pltpu.make_async_copy(src, dst.at[c], o_recv.at[i, c]).wait()

    run = jnp.zeros((1, cols), jnp.float32)
    for j in range(half):
        acc[...] = jnp.zeros_like(acc)
        for c in range(2):
            pltpu.make_async_copy(a, a_slot(c, j), a_recv.at[c, j]).wait()

            def one(slot, carry):
                mask = jnp.where(s2[c, 0:1, :] == slot.astype(jnp.float32), 1.0, 0.0).astype(gt2.dtype)
                p = jnp.dot(
                    gt2[c] * mask,
                    a2[c * rows:(c + 1) * rows, j * cols:(j + 1) * cols],
                    preferred_element_type=jnp.float32,
                )
                acc[...] += p * p
                return carry

            lax.fori_loop(0, slots, one, 0)
        total = acc[...]
        sq[:, j * cols:(j + 1) * cols] = total.astype(sq.dtype)
        run = run + jnp.sum(total, axis=0, keepdims=True)
    sums[...] = jnp.broadcast_to(jnp.sum(run, axis=1, keepdims=True), sums.shape)

    for j in range(half):
        pltpu.make_async_copy(q, q_slot(j), q_recv.at[j]).wait()
    for k in range(1, mp):
        a_copy(k).wait_send()

    @pl.when(owner == core)
    def _():
        for k in range(1, mp):
            q_copy(k).wait_send()

    @pl.when(owner != core)
    def _():
        a_copy(0).wait_send()

    for i, (src, dst) in enumerate(pairs):
        remote(src, dst.at[core], o_send.at[i], o_recv.at[i, core], sibling, m).wait_send()


def spread(mp, slots, a, g, gt, q, s):
    rows, cols = a.shape
    half = mp // 2
    dma = pltpu.SemaphoreType.DMA
    return pl.pallas_call(
        functools.partial(spread_kernel, mp, slots),
        out_shape=[
            jax.ShapeDtypeStruct((2 * rows, half * cols), a.dtype),
            jax.ShapeDtypeStruct((2,) + g.shape, g.dtype),
            jax.ShapeDtypeStruct((q.shape[0], half * cols), q.dtype),
            jax.ShapeDtypeStruct((2,) + s.shape, s.dtype),
            jax.ShapeDtypeStruct((g.shape[1], half * cols), jnp.bfloat16),
            jax.ShapeDtypeStruct((8, 128), jnp.float32),
        ],
        in_specs=[VMEM] * 5,
        out_specs=[VMEM] * 6,
        scratch_shapes=[
            pltpu.VMEM((2,) + gt.shape, gt.dtype),
            pltpu.VMEM((g.shape[1], cols), jnp.float32),
            dma((mp,)), dma((2, half)), dma((mp,)), dma((half,)), dma((3,)), dma((3, 2)),
        ],
        compiler_params=pltpu.CompilerParams(has_side_effects=True, vmem_limit_bytes=GRANT),
        name="spread",
    )(a, g, gt, q, s)


def piece(ref, across, shape, p):
    high, wide = shape
    return ref.at[
        pl.ds(pl.multiple_of((p // across) * high, high), high),
        pl.ds(pl.multiple_of(lax.rem(p, across) * wide, wide), wide),
    ]


def scatter_kernel(n, mp, across, shape, c, t, r, tt, c_send, c_recv, t_send, t_recv, u_send, u_recv):
    d, m = lax.axis_index("dp"), lax.axis_index("mp")
    core = lax.rem(d, 2)
    chip = d // 2
    base = d - core
    near = 2 * mp
    me = core * mp + m

    def c_copy(k):
        p = lax.rem(chip + k, n)
        return remote(piece(c, across, shape, p), r.at[chip], c_send.at[k], c_recv.at[chip], 2 * p + core, m)

    def t_copy(k):
        o = lax.rem(me + k, near)
        return remote(t, tt.at[chip, me], t_send.at[k], t_recv.at[me], base + o // mp, lax.rem(o, mp))

    def u_copy(k):
        p = lax.rem(chip + k, n)
        return remote(tt.at[chip], tt.at[chip], u_send.at[k], u_recv.at[chip], 2 * p + core, m)

    for k in range(1, near):
        t_copy(k).start()
    pltpu.make_async_copy(t, tt.at[chip, me], t_recv.at[me]).start()
    for k in range(1, n):
        c_copy(k).start()
    pltpu.make_async_copy(piece(c, across, shape, chip), r.at[chip], c_recv.at[chip]).start()
    for o in range(near):
        pltpu.make_async_copy(t, tt.at[chip, o], t_recv.at[o]).wait()
    for k in range(1, n):
        u_copy(k).start()
    for k in range(1, near):
        t_copy(k).wait_send()
    for k in range(1, n):
        p = lax.rem(chip + k, n)
        pltpu.make_async_copy(tt.at[chip], tt.at[p], u_recv.at[p]).wait()
        u_copy(k).wait_send()
        c_copy(k).wait_send()
    for p in range(n):
        pltpu.make_async_copy(piece(c, across, shape, chip), r.at[p], c_recv.at[p]).wait()


def scatter(n, mp, across, shape, c, t):
    dma = pltpu.SemaphoreType.DMA
    return pl.pallas_call(
        functools.partial(scatter_kernel, n, mp, across, shape),
        out_shape=[
            jax.ShapeDtypeStruct((n,) + shape, c.dtype),
            jax.ShapeDtypeStruct((n, 2 * mp) + t.shape, t.dtype),
        ],
        in_specs=[VMEM] * 2,
        out_specs=[VMEM] * 2,
        scratch_shapes=[dma((n,)), dma((n,)), dma((2 * mp,)), dma((2 * mp,)), dma((n,)), dma((n,))],
        compiler_params=pltpu.CompilerParams(has_side_effects=True, vmem_limit_bytes=GRANT),
        name="scatter",
    )(c, t)


def collect_kernel(n, across, shape, x, out, send, recv):
    d, m = lax.axis_index("dp"), lax.axis_index("mp")
    core = lax.rem(d, 2)
    chip = d // 2
    here = piece(out, across, shape, chip)

    def copy(k):
        return remote(x, here, send.at[k], recv.at[chip], 2 * lax.rem(chip + k, n) + core, m)

    for k in range(1, n):
        copy(k).start()
    pltpu.make_async_copy(x, here, recv.at[chip]).start()
    for p in range(n):
        pltpu.make_async_copy(x, piece(out, across, shape, p), recv.at[p]).wait()
    for k in range(1, n):
        copy(k).wait_send()


def collect(n, across, shape, full, x):
    dma = pltpu.SemaphoreType.DMA
    return pl.pallas_call(
        functools.partial(collect_kernel, n, across, shape),
        out_shape=jax.ShapeDtypeStruct(full, x.dtype),
        in_specs=[VMEM],
        out_specs=VMEM,
        scratch_shapes=[dma((n,)), dma((n,))],
        compiler_params=pltpu.CompilerParams(has_side_effects=True, vmem_limit_bytes=GRANT),
        name="collect",
    )(x)


def score_kernel(g2, a2, p, out):
    rows = g2.shape[1]

    @pl.when(pl.program_id(0) == 0)
    def _():
        out[...] = jnp.zeros_like(out)

    for c, at in ((0, 0), (1, rows)):
        y = jnp.dot(g2[c], p[...], preferred_element_type=jnp.float32)
        z = y * a2[at:at + rows, :].astype(jnp.float32)
        total = z[:, :128]
        for lane in range(128, z.shape[1], 128):
            total = total + z[:, lane:lane + 128]
        out[at:at + rows, :] += total


def token_scores(g2, a2, p, tile):
    rows2, cols = a2.shape
    whole = lambda j: (0, 0)
    part = lambda j: (0, j)
    return pl.pallas_call(
        score_kernel,
        grid=(cols // tile,),
        out_shape=jax.ShapeDtypeStruct((rows2, 128), jnp.float32),
        in_specs=[
            pl.BlockSpec(g2.shape, lambda j: (0, 0, 0)),
            pl.BlockSpec((rows2, tile), part),
            pl.BlockSpec((p.shape[0], tile), part),
        ],
        out_specs=pl.BlockSpec((rows2, 128), whole),
        compiler_params=pltpu.CompilerParams(vmem_limit_bytes=GRANT),
        name="token_scores",
    )(g2, a2, p)


def finish_kernel(mp, t, out, send, recv):
    d, m = lax.axis_index("dp"), lax.axis_index("mp")
    core = lax.rem(d, 2)
    base = d - core
    near = 2 * mp
    me = core * mp + m

    def copy(k):
        o = lax.rem(me + k, near)
        return remote(t, out.at[me], send.at[k], recv.at[me], base + o // mp, lax.rem(o, mp))

    for k in range(1, near):
        copy(k).start()
    pltpu.make_async_copy(t, out.at[me], recv.at[me]).start()
    for o in range(near):
        pltpu.make_async_copy(t, out.at[o], recv.at[o]).wait()
    for k in range(1, near):
        copy(k).wait_send()


def share(mp, t):
    dma = pltpu.SemaphoreType.DMA
    return pl.pallas_call(
        functools.partial(finish_kernel, mp),
        out_shape=jax.ShapeDtypeStruct((2 * mp,) + t.shape, t.dtype),
        in_specs=[VMEM],
        out_specs=VMEM,
        scratch_shapes=[dma((2 * mp,)), dma((2 * mp,))],
        compiler_params=pltpu.CompilerParams(has_side_effects=True),
        name="share",
    )(t)


def shards(dp, mp, train_acts, train_grads, lengths, query_acts, query_grads, basis_in, basis_out):
    rows = train_acts.shape[0]
    width = basis_in.shape[1]
    slots = lengths.shape[0]
    n = dp // 2
    cols = (mp // 2) * basis_in.shape[1]
    down = max(
        k for k in range(1, n + 1) if n % k == 0 and width % (8 * k) == 0 and cols % (128 * (n // k)) == 0
    )
    across = n // down
    shape = (width // down, cols // across)
    tile = 256
    core = lax.axis_index("dp") % 2
    chip = lax.axis_index("dp") // 2

    finish = jnp.cumsum(lengths)
    slot_of = jnp.sum(jnp.arange(rows, dtype=jnp.int32)[None, :] >= finish[:, None], axis=0)
    slot_rows = jnp.broadcast_to(slot_of.astype(jnp.float32)[None, :], (8, rows))
    acts_block = rotate(train_acts, basis_in)
    grads_own = rotate(train_grads, basis_out)
    query_block = rotate(query_acts, basis_in)
    query_grot = rotate(query_grads, basis_out)
    acts2, grads2, query2, slot2, squared, total = spread(
        mp, slots, acts_block, grads_own, grads_own.T, query_block, slot_rows
    )

    own_first = core == 0
    names = jnp.arange(slots, dtype=jnp.float32)
    mask0 = names[:, None] == slot2[0, 0][None, :]
    mask1 = names[:, None] == slot2[1, 0][None, :]

    pieces, totals = scatter(n, mp, across, shape, squared, total)

    sequences = slots * dp
    curvature = jnp.sum(pieces.astype(jnp.float32), axis=0) / sequences
    entries = width * mp * width * mp
    damping = damping_ratio * (jnp.sum(totals[:, :, 0, 0]) / sequences / entries)
    row_at = (chip // across) * shape[0]
    col_at = (chip % across) * shape[1]
    left = lax.dynamic_slice_in_dim(query_grot, row_at, shape[0], 1)
    right = lax.dynamic_slice_in_dim(query2, col_at, shape[1], 1)
    local_grad = lax.dot_general(left, right, (((0,), (0,)), ((), ())), preferred_element_type=jnp.float32)
    precond = (local_grad / (curvature + damping)).astype(jnp.bfloat16)
    precond_full = collect(n, across, shape, (width, cols), precond)

    by_token = jnp.sum(token_scores(grads2, acts2, precond_full, tile), axis=1)
    partial0 = jnp.sum(jnp.where(mask0, by_token[None, :rows], 0.0), axis=1)
    partial1 = jnp.sum(jnp.where(mask1, by_token[None, rows:], 0.0), axis=1)
    packed = jnp.zeros((8, 128), jnp.float32).at[0, :slots].set(partial0).at[1, :slots].set(partial1)
    summed = jnp.sum(share(mp, packed), axis=0)
    return jnp.where(own_first, summed[0:1, :slots], summed[1:2, :slots])


def solution(mesh):
    return jax.shard_map(
        functools.partial(shards, mesh.shape["dp"], mesh.shape["mp"]),
        mesh=mesh,
        in_specs=(P("dp", None), P("dp", None), P("dp"), P(), P(), P(None, "mp"), P(None, "mp")),
        out_specs=P(None, "dp"),
        check_vma=False,
    )
```
